256 devices in a mesh: data: 256 (over z, y, x, core).
Axes of the slice: x: 4, y: 4, z: 8, core: 2. Of those that a mesh axis runs over, the one named last changes fastest.
Arguments:
- x_step: bfloat16 [2, 512, 256, 384], P(None, 'data')
- labels: int32 [2, 512], P(None, 'data')
- x_next: bfloat16 [512, 256, 384], P('data')
- w_in: float32 [4, 384, 1536], replicated
- w_out: float32 [4, 1536, 384], replicated
- w_head: float32 [384, 1000], replicated
- mom_in: float32 [4, 384, 1536], replicated
- mom_out: float32 [4, 1536, 384], replicated
- mom_head: float32 [384, 1000], replicated
- learn_rate: float32 [], replicated
- mom_coef: float32 [], replicated
Outputs:
- output 1: float32 [512, 1000], P('data')
- output 2: float32 [4, 384, 1536], replicated
- output 3: float32 [4, 1536, 384], replicated
- output 4: float32 [384, 1000], replicated
- output 5: float32 [4, 384, 1536], replicated
- output 6: float32 [4, 1536, 384], replicated
- output 7: float32 [384, 1000], replicated
All inputs are finite; a program needn't handle non-finite values.
Results may differ from the reference program's by a relative error of at most 0.0186965.
Values are sent between devices in bfloat16 or wider.
A program may use at most 768 MiB of HBM per device.

```python
import jax
import jax.numpy as jnp
from jax import lax

D = 384
FF = 1536
SEQ = 256
CLASSES = 1000
LAYERS = 4
BATCH_DEV = 2
GROUP = 256
MICRO = 2
BATCH = GROUP * BATCH_DEV
EXAMPLES = MICRO * BATCH
LN_EPS = 1e-6


def setup_inputs(seed: int = 0) -> dict:
    key_list = jax.random.split(jax.random.key(seed), 13)
    img_step = jax.random.normal(key_list[0], (MICRO, BATCH, 1, D), jnp.float32)
    tok_step = jax.random.normal(key_list[1], (MICRO, BATCH, SEQ, D), jnp.float32)
    img_next = jax.random.normal(key_list[2], (BATCH, 1, D), jnp.float32)
    tok_next = jax.random.normal(key_list[3], (BATCH, SEQ, D), jnp.float32)
    labels = jax.random.randint(key_list[4], (MICRO, BATCH), 0, CLASSES, jnp.int32)
    in_scale = D ** -0.5
    out_scale = FF ** -0.5
    mom_rel = 0.3 * EXAMPLES ** -0.5
    return {
        'x_step': (0.8 * img_step + 0.6 * tok_step).astype(jnp.bfloat16),
        'labels': labels,
        'x_next': (0.8 * img_next + 0.6 * tok_next).astype(jnp.bfloat16),
        'w_in': jax.random.normal(key_list[5], (LAYERS, D, FF), jnp.float32) * in_scale,
        'w_out': jax.random.normal(key_list[6], (LAYERS, FF, D), jnp.float32) * out_scale,
        'w_head': jax.random.normal(key_list[7], (D, CLASSES), jnp.float32) * in_scale,
        'mom_in': jax.random.normal(key_list[8], (LAYERS, D, FF), jnp.float32) * (in_scale * mom_rel),
        'mom_out': jax.random.normal(key_list[9], (LAYERS, FF, D), jnp.float32) * (out_scale * mom_rel),
        'mom_head': jax.random.normal(key_list[10], (D, CLASSES), jnp.float32) * (in_scale * mom_rel),
        'learn_rate': jax.random.uniform(key_list[11], (), jnp.float32, 0.1, 0.2) * EXAMPLES ** 0.5,
        'mom_coef': jax.random.uniform(key_list[12], (), jnp.float32, 0.5, 0.9),
    }


def norm_rows(x_f32):
    row_mean = jnp.mean(x_f32, axis=-1, keepdims=True)
    centered = x_f32 - row_mean
    row_var = jnp.mean(centered * centered, axis=-1, keepdims=True)
    return centered * lax.rsqrt(row_var + LN_EPS)


def block_forward(tok_rows, w_one, w_two):
    x_f32 = tok_rows.astype(jnp.float32)
    normed = norm_rows(x_f32).astype(jnp.bfloat16)
    pre_act = jnp.dot(normed, w_one.astype(jnp.bfloat16), preferred_element_type=jnp.float32)
    hidden = jax.nn.gelu(pre_act).astype(jnp.bfloat16)
    mlp_out = jnp.dot(hidden, w_two.astype(jnp.bfloat16), preferred_element_type=jnp.float32)
    return (x_f32 + mlp_out).astype(jnp.bfloat16)


def image_logits(images, w_in, w_out, w_head):
    n_img = images.shape[0]

    def layer_step(tok_rows, weights):
        return block_forward(tok_rows, weights[0], weights[1]), None

    tok_rows, _ = lax.scan(layer_step, images.reshape(n_img * SEQ, D), (w_in, w_out))
    pooled = jnp.mean(tok_rows.reshape(n_img, SEQ, D), axis=1, dtype=jnp.float32)
    return jnp.dot(pooled.astype(jnp.bfloat16), w_head.astype(jnp.bfloat16), preferred_element_type=jnp.float32)


def group_loss(params, images, lab_row):
    logits = image_logits(images, params[0], params[1], params[2])
    log_prob = jax.nn.log_softmax(logits, axis=-1)
    picked = jnp.take_along_axis(log_prob, lab_row[:, None], axis=-1)
    return -jnp.sum(picked) / EXAMPLES


def reference(x_step, labels, x_next, w_in, w_out, w_head, mom_in, mom_out, mom_head, learn_rate, mom_coef):
    params = (w_in, w_out, w_head)
    img_groups = x_step.reshape(MICRO * GROUP, BATCH_DEV, SEQ, D)
    lab_groups = labels.reshape(MICRO * GROUP, BATCH_DEV)
    grad_fn = jax.grad(group_loss)

    def accumulate(grad_sum, group_in):
        part_grad = grad_fn(params, group_in[0], group_in[1])
        return jax.tree.map(jnp.add, grad_sum, part_grad), None

    zero_grads = jax.tree.map(jnp.zeros_like, params)
    grad_sum, _ = lax.scan(accumulate, zero_grads, (img_groups, lab_groups))
    new_mom_in = mom_coef * mom_in + grad_sum[0]
    new_mom_out = mom_coef * mom_out + grad_sum[1]
    new_mom_head = mom_coef * mom_head + grad_sum[2]
    new_w_in = w_in - learn_rate * new_mom_in
    new_w_out = w_out - learn_rate * new_mom_out
    new_w_head = w_head - learn_rate * new_mom_head
    next_groups = x_next.reshape(GROUP, BATCH_DEV, SEQ, D)
    logits = lax.map(lambda images: image_logits(images, new_w_in, new_w_out, new_w_head), next_groups)
    return (logits.reshape(BATCH, CLASSES), new_w_in, new_w_out, new_w_head, new_mom_in, new_mom_out, new_mom_head)
```

```python
import functools

import jax
import jax.numpy as jnp
from jax import lax
from jax.experimental import pallas as pl
from jax.experimental.pallas import tpu as pltpu
from jax.sharding import PartitionSpec as P

LN_EPS = 1e-6
BF = jnp.bfloat16
F32 = jnp.float32

UR = 16
CHUNKS = 10
STAGES = 13
SEMS = 36


def mod(a, n):
    return lax.rem(a + n, n)


class Reducer:
    def __init__(self, own, full, from_core, rel1, nb1, rel2, nb2, from_z, send_sem, recv_sem):
        self.own, self.full = own, full
        self.from_core, self.rel1, self.nb1 = from_core, rel1, nb1
        self.rel2, self.nb2, self.from_z = rel2, nb2, from_z
        self.send_sem, self.recv_sem = send_sem, recv_sem
        me = lax.axis_index('data')
        self.me = me
        self.core = lax.rem(me, 2)
        self.x = lax.rem(lax.div(me, 2), 4)
        self.y = lax.rem(lax.div(me, 8), 4)
        self.z = lax.div(me, 32)

    @staticmethod
    def scratch():
        dma = pltpu.SemaphoreType.DMA((CHUNKS, SEMS))
        unit = lambda n: pltpu.VMEM((CHUNKS * n, UR, 128), BF)
        return [unit(256), unit(256), unit(128), unit(32), unit(64), unit(8), unit(16), unit(8), dma, dma]

    def peers(self):
        base = self.me - self.z * 32
        x0 = self.me - self.x * 2
        y0 = self.me - self.y * 8
        out = [self.me + 1 - 2 * self.core]
        out += [x0 + 2 * mod(self.x + d, 4) for d in (1, 3)]
        out += [y0 + 8 * mod(self.y + d, 4) for d in (1, 3)]
        out += [base + 32 * mod(self.z + d, 8) for d in range(1, 8)]
        return out

    def greet(self):
        barrier = pltpu.get_barrier_semaphore()
        for peer in self.peers():
            pl.semaphore_signal(barrier, inc=1, device_id=(peer,), device_id_type=pl.DeviceIdType.MESH)

    def meet(self):
        pl.semaphore_wait(pltpu.get_barrier_semaphore(), 12)

    def view(self, c):
        par = lax.rem(c, 2)
        v = {}
        m1 = self.x + par * (self.y - self.x)
        m2 = self.y + par * (self.x - self.y)
        s1 = 2 + par * 6
        s2 = 8 - par * 6
        v['c'] = c
        v['m1'], v['m2'] = m1, m2
        v['r1'], v['l1'] = mod(m1 + 1, 4), mod(m1 + 3, 4)
        v['r2'], v['l2'] = mod(m2 + 1, 4), mod(m2 + 3, 4)
        v['o1'], v['o2'] = mod(m1 + 2, 4), mod(m2 + 2, 4)
        b1 = self.me - m1 * s1
        b2 = self.me - m2 * s2
        v['dr1'], v['dl1'] = b1 + v['r1'] * s1, b1 + v['l1'] * s1
        v['dr2'], v['dl2'] = b2 + v['r2'] * s2, b2 + v['l2'] * s2
        v['base0'] = c * 256 + self.core * 128
        v['base1'] = v['base0'] + m1 * 32
        v['base2'] = v['base1'] + m2 * 8
        return v

    def copy(self, v, k, src, dst, dev):
        return pltpu.make_async_remote_copy(
            src_ref=src, dst_ref=dst,
            send_sem=self.send_sem.at[v['c'], k], recv_sem=self.recv_sem.at[v['c'], k],
            device_id=(dev,), device_id_type=pl.DeviceIdType.MESH)

    def copies(self, s, v):
        own, full, c, z = self.own, self.full, v['c'], self.z
        cp = functools.partial(self.copy, v)
        if s == 0:
            other = c * 256 + (1 - self.core) * 128
            return [cp(0, own.at[pl.ds(other, 128)], self.from_core.at[pl.ds(c * 128, 128)],
                       self.me + 1 - 2 * self.core)]
        if s in (1, 3):
            ring = s == 1
            n = 16 if ring else 4
            base = v['base0'] if ring else v['base1']
            step = 32 if ring else 8
            r, l, o = (v['r1'], v['l1'], v['o1']) if ring else (v['r2'], v['l2'], v['o2'])
            dr, dl = (v['dr1'], v['dl1']) if ring else (v['dr2'], v['dl2'])
            rel, nb, k = (self.rel1, self.nb1, 1) if ring else (self.rel2, self.nb2, 7)
            return [
                cp(k, own.at[pl.ds(base + o * step, n)], rel.at[pl.ds(c * 2 * n, n)], dr),
                cp(k + 1, own.at[pl.ds(base + o * step + n, n)], rel.at[pl.ds(c * 2 * n + n, n)], dl),
                cp(k + 2, own.at[pl.ds(base + r * step + n, n)], nb.at[pl.ds(c * 4 * n + n, n)], dr),
                cp(k + 3, own.at[pl.ds(base + l * step, n)], nb.at[pl.ds(c * 4 * n + 2 * n, n)], dl),
            ]
        if s in (2, 4):
            ring = s == 2
            n = 16 if ring else 4
            base = v['base0'] if ring else v['base1']
            step = 32 if ring else 8
            r, l = (v['r1'], v['l1']) if ring else (v['r2'], v['l2'])
            dr, dl = (v['dr1'], v['dl1']) if ring else (v['dr2'], v['dl2'])
            nb, k = (self.nb1, 5) if ring else (self.nb2, 11)
            return [
                cp(k, own.at[pl.ds(base + r * step, n)], nb.at[pl.ds(c * 4 * n, n)], dr),
                cp(k + 1, own.at[pl.ds(base + l * step + n, n)], nb.at[pl.ds(c * 4 * n + 3 * n, n)], dl),
            ]
        if s == 5:
            zb = self.me - z * 32
            out = []
            for j in range(1, 8):
                to = mod(z + j, 8)
                out.append(cp(12 + j, own.at[pl.ds(v['base2'] + to, 1)],
                              self.from_z.at[pl.ds(c * 8 + j, 1)], zb + to * 32))
            return out
        if s == 6:
            zb = self.me - z * 32
            ref = full.at[pl.ds(v['base2'] + z, 1)]
            return [cp(19 + j, ref, ref, zb + mod(z + j, 8) * 32) for j in range(1, 8)]
        if s == 7:
            ref = full.at[pl.ds(v['base2'], 8)]
            return [cp(27, ref, ref, v['dr2']), cp(28, ref, ref, v['dl2'])]
        if s == 8:
            a = full.at[pl.ds(v['base1'] + v['l2'] * 8, 4)]
            b = full.at[pl.ds(v['base1'] + v['r2'] * 8 + 4, 4)]
            return [cp(29, a, a, v['dr2']), cp(30, b, b, v['dl2'])]
        if s == 9:
            ref = full.at[pl.ds(v['base1'], 32)]
            return [cp(31, ref, ref, v['dr1']), cp(32, ref, ref, v['dl1'])]
        if s == 10:
            a = full.at[pl.ds(v['base0'] + v['l1'] * 32, 16)]
            b = full.at[pl.ds(v['base0'] + v['r1'] * 32 + 16, 16)]
            return [cp(33, a, a, v['dr1']), cp(34, b, b, v['dl1'])]
        ref = full.at[pl.ds(v['base0'], 128)]
        return [cp(35, ref, ref, self.me + 1 - 2 * self.core)]

    def land(self, v, k, ref):
        self.copy(v, k, ref, ref, self.me + 1 - 2 * self.core).wait_recv()

    def arrive(self, s, v):
        own, full, c, z = self.own, self.full, v['c'], self.z
        land = functools.partial(self.land, v)

        def add(at, n, ref, *ats):
            total = own[pl.ds(at, n)].astype(F32)
            for a in ats:
                total = total + ref[pl.ds(a, n)].astype(F32)
            own[pl.ds(at, n)] = total.astype(BF)

        if s == 1:
            land(0, self.from_core.at[pl.ds(c * 128, 128)])
            for q in range(4):
                add(v['base0'] + q * 32, 32, self.from_core, c * 128 + q * 32)
        elif s in (2, 4):
            ring = s == 2
            n = 16 if ring else 4
            base = v['base0'] if ring else v['base1']
            step = 32 if ring else 8
            r, l = (v['r1'], v['l1']) if ring else (v['r2'], v['l2'])
            rel, k = (self.rel1, 1) if ring else (self.rel2, 7)
            land(k, rel.at[pl.ds(c * 2 * n, n)])
            add(base + r * step, n, rel, c * 2 * n)
            land(k + 1, rel.at[pl.ds(c * 2 * n + n, n)])
            add(base + l * step + n, n, rel, c * 2 * n + n)
        elif s in (3, 5):
            ring = s == 3
            n = 16 if ring else 4
            base = v['base1'] if ring else v['base2']
            nb, k = (self.nb1, 1) if ring else (self.nb2, 7)
            for kk, q in ((k + 4, 0), (k + 2, 1), (k + 3, 2), (k + 5, 3)):
                land(kk, nb.at[pl.ds(c * 4 * n + q * n, n)])
            add(base, 2 * n, nb, c * 4 * n, c * 4 * n + 2 * n)
        elif s == 6:
            for j in range(1, 8):
                land(12 + j, self.from_z.at[pl.ds(c * 8 + j, 1)])
            total = own[pl.ds(v['base2'] + z, 1)].astype(F32)
            for j in range(1, 8):
                total = total + self.from_z[pl.ds(c * 8 + j, 1)].astype(F32)
            full[pl.ds(v['base2'] + z, 1)] = total.astype(BF)
        elif s == 7:
            for j in range(1, 8):
                land(19 + j, full.at[pl.ds(v['base2'] + mod(z + 8 - j, 8), 1)])
        elif s == 8:
            land(27, full.at[pl.ds(v['base1'] + v['l2'] * 8, 8)])
            land(28, full.at[pl.ds(v['base1'] + v['r2'] * 8, 8)])
        elif s == 9:
            land(29, full.at[pl.ds(v['base1'] + v['o2'] * 8, 4)])
            land(30, full.at[pl.ds(v['base1'] + v['o2'] * 8 + 4, 4)])
        elif s == 10:
            land(31, full.at[pl.ds(v['base0'] + v['l1'] * 32, 32)])
            land(32, full.at[pl.ds(v['base0'] + v['r1'] * 32, 32)])
        elif s == 11:
            land(33, full.at[pl.ds(v['base0'] + v['o1'] * 32, 16)])
            land(34, full.at[pl.ds(v['base0'] + v['o1'] * 32 + 16, 16)])
        elif s == 12:
            land(35, full.at[pl.ds(c * 256 + (1 - self.core) * 128, 128)])

    def stage(self, s, c):
        v = self.view(c)
        self.arrive(s, v)
        if s < STAGES - 1:
            for copy in self.copies(s, v):
                copy.start()

    def tick(self, t):
        for s in reversed(range(STAGES)):
            c = t - s

            @pl.when(jnp.logical_and(c >= 0, c < CHUNKS))
            def _():
                self.stage(s, c)

    def drain(self):
        def body(c, carry):
            v = self.view(c)
            for s in range(STAGES - 1):
                for copy in self.copies(s, v):
                    copy.wait_send()
            return carry

        lax.fori_loop(0, CHUNKS, body, 0)


HEAD_COLS = 1024


def places(layers, d, ff):
    out = []
    u = 0
    out.append((2 * layers, u, d, HEAD_COLS))
    u += d // UR * (HEAD_COLS // 128)
    for layer in reversed(range(layers)):
        out.append((layer, u, ff, d))
        u += ff // UR * (d // 128)
        out.append((layers + layer, u, d, ff))
        u += d // UR * (ff // 128)
    return out, u


def sum_kernel(layers, d, ff, *refs):
    n = 2 * layers + 1
    ins, outs, scratch = refs[:n], refs[n:2 * n], refs[2 * n:]
    red = Reducer(*scratch)
    red.greet()
    own, full = scratch[0], scratch[1]
    where, used = places(layers, d, ff)
    for idx, u0, rows, cols in where:
        per = rows // UR
        real = ins[idx].shape[1]
        for j in range(cols // 128):
            width = min(128, real - j * 128)
            block = ins[idx][:, j * 128:j * 128 + width].reshape(per, UR, width)
            if width < 128:
                own[pl.ds(u0 + j * per, per)] = jnp.zeros((per, UR, 128), BF)
                own[pl.ds(u0 + j * per, per), :, :width] = block
            else:
                own[pl.ds(u0 + j * per, per)] = block
    own[pl.ds(used, CHUNKS * 256 - used)] = jnp.zeros((CHUNKS * 256 - used, UR, 128), BF)
    red.meet()

    def body(t, carry):
        red.tick(t)
        return carry

    lax.fori_loop(0, CHUNKS + STAGES - 1, body, 0)
    red.drain()
    for idx, u0, rows, cols in where:
        per = rows // UR
        real = outs[idx].shape[1]
        for j in range(cols // 128):
            width = min(128, real - j * 128)
            block = full[pl.ds(u0 + j * per, per)].reshape(rows, 128)
            outs[idx][:, j * 128:j * 128 + width] = block[:, :width]


def sum_over_data(grads, layers, d, ff):
    n = len(grads)
    vmem = pl.BlockSpec(memory_space=pltpu.VMEM)
    return pl.pallas_call(
        functools.partial(sum_kernel, layers, d, ff),
        out_shape=[jax.ShapeDtypeStruct(g.shape, BF) for g in grads],
        in_specs=[vmem] * n,
        out_specs=[vmem] * n,
        scratch_shapes=Reducer.scratch(),
        compiler_params=pltpu.CompilerParams(
            collective_id=0, has_side_effects=True, vmem_limit_bytes=60 * 1024 * 1024),
        name='sum_over_data',
    )(*grads)


def norm_rows(x_f32):
    row_mean = jnp.mean(x_f32, axis=-1, keepdims=True)
    centered = x_f32 - row_mean
    row_var = jnp.mean(centered * centered, axis=-1, keepdims=True)
    return centered * lax.rsqrt(row_var + LN_EPS)


def block_forward(tok_act, w_one, w_two):
    x_f32 = tok_act.astype(F32)
    normed = norm_rows(x_f32).astype(BF)
    pre_act = jnp.einsum('sd,df->sf', normed, w_one, preferred_element_type=F32)
    hidden = jax.nn.gelu(pre_act).astype(BF)
    mlp_out = jnp.einsum('sf,fd->sd', hidden, w_two, preferred_element_type=F32)
    return (x_f32 + mlp_out).astype(BF), (normed, pre_act, hidden)


def block_backward(tok_act, saved_act, d_out, w_one, w_two, need_input):
    normed, pre_act, hidden = saved_act
    d_out_b = d_out.astype(BF)
    g_two = jnp.einsum('sf,sd->fd', hidden, d_out_b, preferred_element_type=F32)
    d_hidden = jnp.einsum('sd,fd->sf', d_out_b, w_two, preferred_element_type=F32)
    _, gelu_back = jax.vjp(jax.nn.gelu, pre_act)
    d_pre = gelu_back(d_hidden)[0].astype(BF)
    g_one = jnp.einsum('sd,sf->df', normed, d_pre, preferred_element_type=F32)
    if not need_input:
        return g_one, g_two, d_out
    d_normed = jnp.einsum('sf,df->sd', d_pre, w_one, preferred_element_type=F32)
    _, norm_back = jax.vjp(norm_rows, tok_act.astype(F32))
    return g_one, g_two, d_out + norm_back(d_normed)[0]


def head_logits(tok_act, n_img, w_head_b):
    seq = tok_act.shape[0] // n_img
    pooled = jnp.mean(tok_act.reshape(n_img, seq, -1), axis=1, dtype=F32).astype(BF)
    return pooled, jnp.dot(pooled, w_head_b, preferred_element_type=F32)


def head_backward(tok_act, lab_row, w_head_b, examples):
    n_img = lab_row.shape[0]
    seq = tok_act.shape[0] // n_img
    pooled, logits = head_logits(tok_act, n_img, w_head_b)
    soft_prob = jax.nn.softmax(logits, axis=-1)
    onehot = (lab_row[:, None] == jnp.arange(logits.shape[1])[None, :]).astype(F32)
    d_logits = ((soft_prob - onehot) / examples).astype(BF)
    g_head = jnp.einsum('bd,bc->dc', pooled, d_logits, preferred_element_type=F32)
    d_pooled = jnp.einsum('bc,dc->bd', d_logits, w_head_b, preferred_element_type=F32)
    d_top = jnp.broadcast_to((d_pooled / seq)[:, None, :], (n_img, seq, tok_act.shape[1]))
    return g_head, d_top.reshape(tok_act.shape)


def solution(mesh):
    group_size = mesh.shape['data']

    def local_step(x_step, labels, x_next, w_in, w_out, w_head, mom_in, mom_out, mom_head, learn_rate, mom_coef):
        micro_count, n_img, seq, d = x_step.shape
        layers, _, ff = w_in.shape
        examples = micro_count * n_img * group_size
        w_in_b = w_in.astype(BF)
        w_out_b = w_out.astype(BF)
        w_head_b = w_head.astype(BF)
        tok_act = x_step.reshape(micro_count * n_img * seq, d)
        kept_in, kept_act = [], []
        for layer_idx in range(layers):
            kept_in.append(tok_act)
            tok_act, saved_act = block_forward(tok_act, w_in_b[layer_idx], w_out_b[layer_idx])
            kept_act.append(saved_act)
        g_head, d_act = head_backward(tok_act, labels.reshape(-1), w_head_b, examples)
        g_in, g_out = [None] * layers, [None] * layers
        for layer_idx in reversed(range(layers)):
            g_in[layer_idx], g_out[layer_idx], d_act = block_backward(
                kept_in[layer_idx], kept_act[layer_idx], d_act, w_in_b[layer_idx], w_out_b[layer_idx], layer_idx > 0)
        grads = [g.astype(BF) for g in g_out + g_in + [g_head]]
        sums = sum_over_data(grads, layers, d, ff)
        red_out, red_in, red_head = sums[:layers], sums[layers:2 * layers], sums[-1]
        new_mom_in = mom_coef * mom_in + jnp.stack(red_in).astype(F32)
        new_mom_out = mom_coef * mom_out + jnp.stack(red_out).astype(F32)
        new_mom_head = mom_coef * mom_head + red_head.astype(F32)
        new_w_in = w_in - learn_rate * new_mom_in
        new_w_out = w_out - learn_rate * new_mom_out
        new_w_head = w_head - learn_rate * new_mom_head
        tok = x_next.reshape(-1, d)
        nwi, nwo = new_w_in.astype(BF), new_w_out.astype(BF)
        for layer_idx in range(layers):
            tok, _ = block_forward(tok, nwi[layer_idx], nwo[layer_idx])
        logits = head_logits(tok, x_next.shape[0], new_w_head.astype(BF))[1]
        return logits, new_w_in, new_w_out, new_w_head, new_mom_in, new_mom_out, new_mom_head

    rep3 = P(None, None, None)
    rep2 = P(None, None)
    return jax.shard_map(
        local_step, mesh=mesh,
        in_specs=(P(None, 'data', None, None), P(None, 'data'), P('data', None, None),
                  rep3, rep3, rep2, rep3, rep3, rep2, P(), P()),
        out_specs=(P('data', None), rep3, rep3, rep2, rep3, rep3, rep2),
        check_vma=False)
```

```python
import functools

import jax
import jax.numpy as jnp
from jax import lax
from jax.experimental import pallas as pl
from jax.experimental.pallas import tpu as pltpu
from jax.sharding import PartitionSpec as P

LN_EPS = 1e-6
BF = jnp.bfloat16
F32 = jnp.float32

UR = 16
CHUNKS = 10
STAGES = 13
LAST_TICK = 16 + STAGES - 1
SEMS = 36


def mod(a, n):
    return lax.rem(a + n, n)


class Reducer:
    def __init__(self, own, full, from_core, rel1, nb1, rel2, nb2, from_z, send_sem, recv_sem, out_sem, result):
        self.out_sem, self.result = out_sem, result
        self.own, self.full = own, full
        self.from_core, self.rel1, self.nb1 = from_core, rel1, nb1
        self.rel2, self.nb2, self.from_z = rel2, nb2, from_z
        self.send_sem, self.recv_sem = send_sem, recv_sem
        me = lax.axis_index('data')
        self.me = me
        self.core = lax.rem(me, 2)
        self.x = lax.rem(lax.div(me, 2), 4)
        self.y = lax.rem(lax.div(me, 8), 4)
        self.z = lax.div(me, 32)

    @staticmethod
    def scratch():
        dma = pltpu.SemaphoreType.DMA((CHUNKS, SEMS))
        unit = lambda n: pltpu.VMEM((CHUNKS * n, UR, 128), BF)
        return [unit(256), unit(256), unit(128), unit(32), unit(64), unit(8), unit(16), unit(8), dma, dma,
                pltpu.SemaphoreType.DMA((CHUNKS,))]

    def peers(self):
        base = self.me - self.z * 32
        x0 = self.me - self.x * 2
        y0 = self.me - self.y * 8
        out = [self.me + 1 - 2 * self.core]
        out += [x0 + 2 * mod(self.x + d, 4) for d in (1, 3)]
        out += [y0 + 8 * mod(self.y + d, 4) for d in (1, 3)]
        out += [base + 32 * mod(self.z + d, 8) for d in range(1, 8)]
        return out

    def greet(self):
        barrier = pltpu.get_barrier_semaphore()
        for peer in self.peers():
            pl.semaphore_signal(barrier, inc=1, device_id=(peer,), device_id_type=pl.DeviceIdType.MESH)

    def meet(self):
        pl.semaphore_wait(pltpu.get_barrier_semaphore(), 12)

    def view(self, c):
        par = lax.rem(c, 2)
        v = {}
        m1 = self.x + par * (self.y - self.x)
        m2 = self.y + par * (self.x - self.y)
        s1 = 2 + par * 6
        s2 = 8 - par * 6
        v['c'] = c
        v['m1'], v['m2'] = m1, m2
        v['r1'], v['l1'] = mod(m1 + 1, 4), mod(m1 + 3, 4)
        v['r2'], v['l2'] = mod(m2 + 1, 4), mod(m2 + 3, 4)
        v['o1'], v['o2'] = mod(m1 + 2, 4), mod(m2 + 2, 4)
        b1 = self.me - m1 * s1
        b2 = self.me - m2 * s2
        v['dr1'], v['dl1'] = b1 + v['r1'] * s1, b1 + v['l1'] * s1
        v['dr2'], v['dl2'] = b2 + v['r2'] * s2, b2 + v['l2'] * s2
        v['base0'] = c * 256 + self.core * 128
        v['base1'] = v['base0'] + m1 * 32
        v['base2'] = v['base1'] + m2 * 8
        return v

    def copy(self, v, k, src, dst, dev):
        return pltpu.make_async_remote_copy(
            src_ref=src, dst_ref=dst,
            send_sem=self.send_sem.at[v['c'], k], recv_sem=self.recv_sem.at[v['c'], k],
            device_id=(dev,), device_id_type=pl.DeviceIdType.MESH)

    def copies(self, s, v):
        own, full, c, z = self.own, self.full, v['c'], self.z
        cp = functools.partial(self.copy, v)
        if s == 0:
            other = c * 256 + (1 - self.core) * 128
            return [cp(0, own.at[pl.ds(other, 128)], self.from_core.at[pl.ds(c * 128, 128)],
                       self.me + 1 - 2 * self.core)]
        if s in (1, 3):
            ring = s == 1
            n = 16 if ring else 4
            base = v['base0'] if ring else v['base1']
            step = 32 if ring else 8
            r, l, o = (v['r1'], v['l1'], v['o1']) if ring else (v['r2'], v['l2'], v['o2'])
            dr, dl = (v['dr1'], v['dl1']) if ring else (v['dr2'], v['dl2'])
            rel, nb, k = (self.rel1, self.nb1, 1) if ring else (self.rel2, self.nb2, 7)
            return [
                cp(k, own.at[pl.ds(base + o * step, n)], rel.at[pl.ds(c * 2 * n, n)], dr),
                cp(k + 1, own.at[pl.ds(base + o * step + n, n)], rel.at[pl.ds(c * 2 * n + n, n)], dl),
                cp(k + 2, own.at[pl.ds(base + r * step + n, n)], nb.at[pl.ds(c * 4 * n + n, n)], dr),
                cp(k + 3, own.at[pl.ds(base + l * step, n)], nb.at[pl.ds(c * 4 * n + 2 * n, n)], dl),
            ]
        if s in (2, 4):
            ring = s == 2
            n = 16 if ring else 4
            base = v['base0'] if ring else v['base1']
            step = 32 if ring else 8
            r, l = (v['r1'], v['l1']) if ring else (v['r2'], v['l2'])
            dr, dl = (v['dr1'], v['dl1']) if ring else (v['dr2'], v['dl2'])
            nb, k = (self.nb1, 5) if ring else (self.nb2, 11)
            return [
                cp(k, own.at[pl.ds(base + r * step, n)], nb.at[pl.ds(c * 4 * n, n)], dr),
                cp(k + 1, own.at[pl.ds(base + l * step + n, n)], nb.at[pl.ds(c * 4 * n + 3 * n, n)], dl),
            ]
        if s == 5:
            zb = self.me - z * 32
            out = []
            for j in range(1, 8):
                to = mod(z + j, 8)
                out.append(cp(12 + j, own.at[pl.ds(v['base2'] + to, 1)],
                              self.from_z.at[pl.ds(c * 8 + j, 1)], zb + to * 32))
            return out
        if s == 6:
            zb = self.me - z * 32
            ref = full.at[pl.ds(v['base2'] + z, 1)]
            return [cp(19 + j, ref, ref, zb + mod(z + j, 8) * 32) for j in range(1, 8)]
        if s == 7:
            ref = full.at[pl.ds(v['base2'], 8)]
            return [cp(27, ref, ref, v['dr2']), cp(28, ref, ref, v['dl2'])]
        if s == 8:
            a = full.at[pl.ds(v['base1'] + v['l2'] * 8, 4)]
            b = full.at[pl.ds(v['base1'] + v['r2'] * 8 + 4, 4)]
            return [cp(29, a, a, v['dr2']), cp(30, b, b, v['dl2'])]
        if s == 9:
            ref = full.at[pl.ds(v['base1'], 32)]
            return [cp(31, ref, ref, v['dr1']), cp(32, ref, ref, v['dl1'])]
        if s == 10:
            a = full.at[pl.ds(v['base0'] + v['l1'] * 32, 16)]
            b = full.at[pl.ds(v['base0'] + v['r1'] * 32 + 16, 16)]
            return [cp(33, a, a, v['dr1']), cp(34, b, b, v['dl1'])]
        ref = full.at[pl.ds(v['base0'], 128)]
        return [cp(35, ref, ref, self.me + 1 - 2 * self.core)]

    def land(self, v, k, ref):
        self.copy(v, k, ref, ref, self.me + 1 - 2 * self.core).wait_recv()

    def arrive(self, s, v):
        own, full, c, z = self.own, self.full, v['c'], self.z
        land = functools.partial(self.land, v)

        def add(at, n, ref, *ats):
            total = own[pl.ds(at, n)].astype(F32)
            for a in ats:
                total = total + ref[pl.ds(a, n)].astype(F32)
            own[pl.ds(at, n)] = total.astype(BF)

        if s == 1:
            land(0, self.from_core.at[pl.ds(c * 128, 128)])
            for q in range(4):
                add(v['base0'] + q * 32, 32, self.from_core, c * 128 + q * 32)
        elif s in (2, 4):
            ring = s == 2
            n = 16 if ring else 4
            base = v['base0'] if ring else v['base1']
            step = 32 if ring else 8
            r, l = (v['r1'], v['l1']) if ring else (v['r2'], v['l2'])
            rel, k = (self.rel1, 1) if ring else (self.rel2, 7)
            land(k, rel.at[pl.ds(c * 2 * n, n)])
            add(base + r * step, n, rel, c * 2 * n)
            land(k + 1, rel.at[pl.ds(c * 2 * n + n, n)])
            add(base + l * step + n, n, rel, c * 2 * n + n)
        elif s in (3, 5):
            ring = s == 3
            n = 16 if ring else 4
            base = v['base1'] if ring else v['base2']
            nb, k = (self.nb1, 1) if ring else (self.nb2, 7)
            for kk, q in ((k + 4, 0), (k + 2, 1), (k + 3, 2), (k + 5, 3)):
                land(kk, nb.at[pl.ds(c * 4 * n + q * n, n)])
            add(base, 2 * n, nb, c * 4 * n, c * 4 * n + 2 * n)
        elif s == 6:
            for j in range(1, 8):
                land(12 + j, self.from_z.at[pl.ds(c * 8 + j, 1)])
            total = own[pl.ds(v['base2'] + z, 1)].astype(F32)
            for j in range(1, 8):
                total = total + self.from_z[pl.ds(c * 8 + j, 1)].astype(F32)
            full[pl.ds(v['base2'] + z, 1)] = total.astype(BF)
        elif s == 7:
            for j in range(1, 8):
                land(19 + j, full.at[pl.ds(v['base2'] + mod(z + 8 - j, 8), 1)])
        elif s == 8:
            land(27, full.at[pl.ds(v['base1'] + v['l2'] * 8, 8)])
            land(28, full.at[pl.ds(v['base1'] + v['r2'] * 8, 8)])
        elif s == 9:
            land(29, full.at[pl.ds(v['base1'] + v['o2'] * 8, 4)])
            land(30, full.at[pl.ds(v['base1'] + v['o2'] * 8 + 4, 4)])
        elif s == 10:
            land(31, full.at[pl.ds(v['base0'] + v['l1'] * 32, 32)])
            land(32, full.at[pl.ds(v['base0'] + v['r1'] * 32, 32)])
        elif s == 11:
            land(33, full.at[pl.ds(v['base0'] + v['o1'] * 32, 16)])
            land(34, full.at[pl.ds(v['base0'] + v['o1'] * 32 + 16, 16)])
        elif s == 12:
            land(35, full.at[pl.ds(c * 256 + (1 - self.core) * 128, 128)])

    def stage(self, s, c):
        v = self.view(c)
        self.arrive(s, v)
        if s < STAGES - 1:
            for copy in self.copies(s, v):
                copy.start()

    def tick(self, t):
        for s in reversed(range(STAGES)):
            u = t - s
            phase = lax.rem(u + 64, 4)
            extra = jnp.logical_or(u == 4, u == 16)
            plain = jnp.logical_and(jnp.logical_and(u >= 2, u < 16), phase >= 2)
            quarter = lax.div(u + 64, 4) - 16
            c_plain = 2 * quarter + phase - 2 + (u > 4).astype(jnp.int32)
            c_extra = 2 + 7 * (u > 4).astype(jnp.int32)
            is_extra = extra.astype(jnp.int32)
            c = is_extra * c_extra + (1 - is_extra) * c_plain

            @pl.when(jnp.logical_or(extra, plain))
            def _():
                self.stage(s, c)
                if s == STAGES - 1:
                    self.finish(c)

    def finish(self, c):
        rows = pl.ds(c * 256, 256)
        pltpu.make_async_copy(self.full.at[rows], self.result.at[rows], self.out_sem.at[c]).start()

    def drain(self):
        def body(c, carry):
            v = self.view(c)
            for s in range(STAGES - 1):
                for copy in self.copies(s, v):
                    copy.wait_send()
            rows = pl.ds(c * 256, 256)
            pltpu.make_async_copy(self.full.at[rows], self.result.at[rows], self.out_sem.at[c]).wait()
            return carry

        lax.fori_loop(0, CHUNKS, body, 0)


SEQ = 256
D = 384
FF = 1536
LAYERS = 4
CLASSES = 1000
IMGS = 4
TOK = IMGS * SEQ
FB = 384
HALF_IN = D // 2
HALF_OUT = FF // 2
GELU_K = 0.7978845608028654
GELU_A = 0.044715

UNITS_HEAD = D // UR * 8
UNITS_ARRAY = D * FF // (UR * 128)
UNITS_USED = UNITS_HEAD + 2 * LAYERS * UNITS_ARRAY


def units_out(layer):
    return UNITS_HEAD + (LAYERS - 1 - layer) * 2 * UNITS_ARRAY


def dot(a, b):
    return lax.dot_general(a, b, (((1,), (0,)), ((), ())), preferred_element_type=F32)


def dot_t(a, b):
    return lax.dot_general(a, b, (((1,), (1,)), ((), ())), preferred_element_type=F32)


def norm_parts(x):
    mean = jnp.mean(x, axis=-1, keepdims=True)
    cent = x - mean
    var = jnp.mean(cent * cent, axis=-1, keepdims=True)
    rstd = lax.rsqrt(var + LN_EPS)
    return cent * rstd, rstd


def gelu(pre):
    return 0.5 * pre * (1.0 + jnp.tanh(GELU_K * (pre + GELU_A * (pre * pre * pre))))


def gelu_and_slope(pre):
    sq = pre * pre
    t = jnp.tanh(GELU_K * pre * (1.0 + GELU_A * sq))
    half = 0.5 * (1.0 + t)
    slope = half + (0.5 * GELU_K) * pre * (1.0 - t * t) * (1.0 + (3.0 * GELU_A) * sq)
    return pre * half, slope


def block_out(x, w_in_of, w_out_of):
    normed = norm_parts(x)[0].astype(BF)
    out = x
    mlp = None
    for f in range(FF // FB):
        hid = gelu(dot(normed, w_in_of(f))).astype(BF)
        part = dot(hid, w_out_of(f))
        mlp = part if mlp is None else mlp + part
    return out + mlp


def step_kernel(x_hbm, lab_ref, w_in, w_out, w_head, result,
                own, full, from_core, rel1, nb1, rel2, nb2, from_z, send_sem, recv_sem, out_sem,
                xs, wi, wo, wh, st_in, st_out, st_head, ht, dp, nt, db, d_act, pooled, ld_sem):
    red = Reducer(own, full, from_core, rel1, nb1, rel2, nb2, from_z, send_sem, recv_sem, out_sem, result)

    def load_in(layer, half):
        return pltpu.make_async_copy(w_in.at[layer, pl.ds(half * HALF_IN, HALF_IN)], st_in.at[half], ld_sem.at[half])

    def load_out(layer, half):
        return pltpu.make_async_copy(w_out.at[layer, pl.ds(half * HALF_OUT, HALF_OUT)], st_out.at[half], ld_sem.at[2 + half])

    load_x = pltpu.make_async_copy(x_hbm, xs.at[pl.ds(0, TOK)], ld_sem.at[4])
    load_head = pltpu.make_async_copy(w_head, st_head, ld_sem.at[5])
    load_x.start()
    for half in range(2):
        load_in(0, half).start()
    for half in range(2):
        load_out(0, half).start()
    load_head.start()
    red.greet()
    own[pl.ds(UNITS_USED, CHUNKS * 256 - UNITS_USED)] = jnp.zeros((CHUNKS * 256 - UNITS_USED, UR, 128), BF)
    pooled[...] = jnp.zeros_like(pooled)
    load_x.wait()

    def fwd_layer(layer, carry):
        for half in range(2):
            load_in(layer, half).wait()
            wi[pl.ds(layer * D + half * HALF_IN, HALF_IN)] = st_in[half].astype(BF)
        for half in range(2):
            load_out(layer, half).wait()
            wo[pl.ds(layer * FF + half * HALF_OUT, HALF_OUT)] = st_out[half].astype(BF)

        @pl.when(layer < LAYERS - 1)
        def _():
            for half in range(2):
                load_in(layer + 1, half).start()
            for half in range(2):
                load_out(layer + 1, half).start()

        def block(i, carry):
            x = xs[pl.ds(layer * TOK + i * SEQ, SEQ)].astype(F32)
            out = block_out(
                x,
                lambda f: wi[pl.ds(layer * D, D), f * FB:(f + 1) * FB],
                lambda f: wo[pl.ds(layer * FF + f * FB, FB)])
            xs[pl.ds((layer + 1) * TOK + i * SEQ, SEQ)] = out.astype(BF)
            return carry

        return lax.fori_loop(0, IMGS, block, carry)

    lax.fori_loop(0, LAYERS, fwd_layer, 0)

    for i in range(IMGS):
        top = xs[pl.ds(LAYERS * TOK + i * SEQ, SEQ)].astype(F32)
        pooled[i:i + 1] = jnp.sum(top, axis=0, keepdims=True) * (1.0 / SEQ)
    load_head.wait()
    wh[...] = st_head[...].astype(BF)
    pool_b = pooled[...].astype(BF)
    logits = dot(pool_b, wh[...])
    ex = jnp.exp(logits - jnp.max(logits, axis=-1, keepdims=True))
    prob = ex / jnp.sum(ex, axis=-1, keepdims=True)
    classes = lax.broadcasted_iota(jnp.int32, logits.shape, 1)
    onehot = (classes == lab_ref[...]).astype(F32)
    examples = IMGS * lax.axis_size('data')
    d_logits = ((prob - onehot) * (1.0 / examples)).astype(BF)
    per = D // UR
    g_head = dot(pooled[...].T.astype(BF), d_logits).astype(BF)
    for j in range(8):
        width = min(128, CLASSES - j * 128)
        part = g_head[:, j * 128:j * 128 + width].reshape(per, UR, width)
        if width < 128:
            own[pl.ds(j * per, per)] = jnp.zeros((per, UR, 128), BF)
            own[pl.ds(j * per, per), :, :width] = part
        else:
            own[pl.ds(j * per, per)] = part
    d_pooled = dot_t(d_logits, wh[...]) * (1.0 / SEQ)
    for i in range(IMGS):
        d_act[i * SEQ:(i + 1) * SEQ] = jnp.broadcast_to(d_pooled[i:i + 1], (SEQ, D))

    red.meet()

    def bwd_layer(li, carry):
        layer = LAYERS - 1 - li
        t0 = li * 4

        def block(i, carry):
            rows = pl.ds(pl.multiple_of(i * SEQ, SEQ), SEQ)
            y, rstd = norm_parts(xs[pl.ds(layer * TOK + i * SEQ, SEQ)].astype(F32))
            normed = y.astype(BF)
            d_out = d_act[rows]
            d_out_b = d_out.astype(BF)
            db[rows] = d_out_b
            nt[:, rows] = normed.T
            d_norm = None
            for f in range(FF // FB):
                cols = slice(f * FB, (f + 1) * FB)
                w1 = wi[pl.ds(layer * D, D), cols]
                hid, slope = gelu_and_slope(dot(normed, w1))
                ht[cols, rows] = hid.astype(BF).T
                d_hid = dot_t(d_out_b, wo[pl.ds(layer * FF + f * FB, FB)])
                d_pre = (d_hid * slope).astype(BF)
                dp[rows, cols] = d_pre
                part = dot_t(d_pre, w1)
                d_norm = part if d_norm is None else d_norm + part
            m1 = jnp.mean(d_norm, axis=-1, keepdims=True)
            m2 = jnp.mean(d_norm * y, axis=-1, keepdims=True)
            d_act[rows] = d_out + rstd * (d_norm - m1 - y * m2)
            return carry

        lax.fori_loop(0, 2, block, 0)
        red.tick(t0)
        lax.fori_loop(2, 4, block, 0)
        red.tick(t0 + 1)
        u_out = UNITS_HEAD + li * (2 * UNITS_ARRAY)
        u_in = u_out + UNITS_ARRAY

        def grad_out(f, carry):
            g = dot(ht[pl.ds(f * FB, FB)], db[...]).astype(BF)
            for j in range(D // 128):
                own[pl.ds(u_out + j * (FF // UR) + f * (FB // UR), FB // UR)] = (
                    g[:, j * 128:(j + 1) * 128].reshape(FB // UR, UR, 128))
            return carry

        def grad_in(f, carry):
            g = dot(nt[...], dp[:, pl.ds(pl.multiple_of(f * FB, FB), FB)]).astype(BF)
            for j in range(FB // 128):
                own[pl.ds(u_in + (f * (FB // 128) + j) * per, per)] = (
                    g[:, j * 128:(j + 1) * 128].reshape(per, UR, 128))
            return carry

        lax.fori_loop(0, FF // FB, grad_out, 0)
        red.tick(t0 + 2)
        lax.fori_loop(0, FF // FB, grad_in, 0)
        red.tick(t0 + 3)
        return carry

    lax.fori_loop(0, LAYERS, bwd_layer, 0)

    def rest(t, carry):
        red.tick(t)
        return carry

    lax.fori_loop(4 * LAYERS, LAST_TICK + 1, rest, 0)
    red.drain()


def summed_gradients(x, labels, w_in, w_out, w_head):
    any_space = pl.BlockSpec(memory_space=pl.ANY)
    vmem = pl.BlockSpec(memory_space=pltpu.VMEM)
    return pl.pallas_call(
        step_kernel,
        out_shape=jax.ShapeDtypeStruct((CHUNKS * 256, UR, 128), BF),
        in_specs=[any_space, vmem, any_space, any_space, any_space],
        out_specs=any_space,
        scratch_shapes=Reducer.scratch() + [
            pltpu.VMEM(((LAYERS + 1) * TOK, D), BF),
            pltpu.VMEM((LAYERS * D, FF), BF),
            pltpu.VMEM((LAYERS * FF, D), BF),
            pltpu.VMEM((D, CLASSES), BF),
            pltpu.VMEM((2, HALF_IN, FF), F32),
            pltpu.VMEM((2, HALF_OUT, D), F32),
            pltpu.VMEM((D, CLASSES), F32),
            pltpu.VMEM((FF, TOK), BF),
            pltpu.VMEM((TOK, FF), BF),
            pltpu.VMEM((D, TOK), BF),
            pltpu.VMEM((TOK, D), BF),
            pltpu.VMEM((TOK, D), F32),
            pltpu.VMEM((16, D), F32),
            pltpu.SemaphoreType.DMA((6,)),
        ],
        compiler_params=pltpu.CompilerParams(
            collective_id=0, has_side_effects=True, vmem_limit_bytes=67043328),
        name='step_and_sum',
    )(x, labels, w_in, w_out, w_head)


SLOTS = 3
N_IMG = 2


def next_kernel(g_hbm, x_hbm, w_in, m_in, w_out, m_out, w_head, m_head, lr_ref, coef_ref,
                logits, nw_in, nm_in, nw_out, nm_out, nw_head, nm_head,
                g, toks, b_wi, b_mi, b_wo, b_mo, b_wh, b_mh, wi, wo, wh, pooled, g_sem, in_sem, out_sem):
    lr, coef = lr_ref[0], coef_ref[0]

    def fetch_g(k, at, n):
        return pltpu.make_async_copy(g_hbm.at[pl.ds(at, n)], g.at[pl.ds(at, n)], g_sem.at[k])

    g_layers = [fetch_g(layer, units_out(layer), 2 * UNITS_ARRAY) for layer in range(LAYERS)]
    g_head = fetch_g(LAYERS, 0, UNITS_HEAD)
    pairs_in = [[pltpu.make_async_copy(src.at[layer], dst.at[layer % SLOTS], in_sem.at[layer, k])
                 for k, (src, dst) in enumerate(((w_in, b_wi), (m_in, b_mi), (w_out, b_wo), (m_out, b_mo)))]
                for layer in range(LAYERS)]
    pairs_out = [[pltpu.make_async_copy(src.at[layer % SLOTS], dst.at[layer], out_sem.at[layer, k])
                  for k, (dst, src) in enumerate(((nw_in, b_wi), (nm_in, b_mi), (nw_out, b_wo), (nm_out, b_mo)))]
                 for layer in range(LAYERS)]
    head_in = [pltpu.make_async_copy(w_head, b_wh, in_sem.at[LAYERS, 0]),
               pltpu.make_async_copy(m_head, b_mh, in_sem.at[LAYERS, 1])]
    head_out = [pltpu.make_async_copy(b_wh, nw_head, out_sem.at[LAYERS, 0]),
                pltpu.make_async_copy(b_mh, nm_head, out_sem.at[LAYERS, 1])]
    load_x = pltpu.make_async_copy(x_hbm, toks, g_sem.at[LAYERS + 1])

    for layer in range(SLOTS):
        g_layers[layer].start()
        for c in pairs_in[layer]:
            c.start()
        if layer == 0:
            load_x.start()
    g_head.start()
    for c in head_in:
        c.start()
    g_layers[SLOTS].start()
    pooled[...] = jnp.zeros_like(pooled)

    def update(b_w, b_m, cast, slot, rows, col, width, grad):
        cols = slice(col, col + width)
        mom = coef * b_m[slot, rows, cols] + grad.astype(F32)
        new = b_w[slot, rows, cols] - lr * mom
        b_m[slot, rows, cols] = mom
        b_w[slot, rows, cols] = new
        cast[rows, cols] = new.astype(BF)

    for layer in range(LAYERS):
        slot = layer % SLOTS
        u_out = units_out(layer)
        u_in = u_out + UNITS_ARRAY
        pin, pout = pairs_in[layer], pairs_out[layer]
        g_layers[layer].wait()
        pin[0].wait()
        pin[1].wait()

        def band_in(r, carry):
            rows = pl.ds(pl.multiple_of(r * UR, UR), UR)
            for j in range(FF // 128):
                update(b_wi, b_mi, wi, slot, rows, j * 128, 128, g[u_in + j * (D // UR) + r])
            return carry

        lax.fori_loop(0, D // UR, band_in, 0)
        pout[0].start()
        pout[1].start()
        pin[2].wait()
        pin[3].wait()

        def band_out(q, carry):
            for e in range(4):
                r = q * 4 + e
                rows = pl.ds(pl.multiple_of(r * UR, UR), UR)
                for j in range(D // 128):
                    update(b_wo, b_mo, wo, slot, rows, j * 128, 128, g[u_out + j * (FF // UR) + r])
            return carry

        lax.fori_loop(0, FF // UR // 4, band_out, 0)
        pout[2].start()
        pout[3].start()
        if layer == 0:
            load_x.wait()

        def block(i, carry):
            rows = pl.ds(pl.multiple_of(i * SEQ, SEQ), SEQ)
            out = block_out(toks[rows].astype(F32),
                            lambda f: wi[:, f * FB:(f + 1) * FB], lambda f: wo[f * FB:(f + 1) * FB])
            toks[rows] = out.astype(BF)
            return carry

        lax.fori_loop(0, N_IMG, block, 0)
        nxt = layer + SLOTS - 1
        if layer >= 1 and nxt < LAYERS:
            for c in pairs_out[layer - 1]:
                c.wait()
            for c in pairs_in[nxt]:
                c.start()

    g_head.wait()
    for c in head_in:
        c.wait()

    def band_head(r, carry):
        rows = pl.ds(pl.multiple_of(r * UR, UR), UR)
        for j in range(8):
            width = min(128, CLASSES - j * 128)
            cols = slice(j * 128, j * 128 + width)
            mom = coef * b_mh[rows, cols] + g[j * (D // UR) + r][:, :width].astype(F32)
            new = b_wh[rows, cols] - lr * mom
            b_mh[rows, cols] = mom
            b_wh[rows, cols] = new
            wh[rows, cols] = new.astype(BF)
        return carry

    lax.fori_loop(0, D // UR, band_head, 0)
    for c in head_out:
        c.start()
    for i in range(N_IMG):
        top = toks[i * SEQ:(i + 1) * SEQ].astype(F32)
        pooled[i:i + 1] = jnp.sum(top, axis=0, keepdims=True) * (1.0 / SEQ)
    logits[...] = dot(pooled[...].astype(BF), wh[...])[:N_IMG]
    for layer in range(LAYERS):
        if layer >= LAYERS - SLOTS:
            for c in pairs_out[layer]:
                c.wait()
    for c in head_out:
        c.wait()


def update_and_next(g, x, w_in, m_in, w_out, m_out, w_head, m_head, lr, coef):
    any_space = pl.BlockSpec(memory_space=pl.ANY)
    smem = pl.BlockSpec(memory_space=pltpu.SMEM)
    vmem = pl.BlockSpec(memory_space=pltpu.VMEM)
    like = lambda a: jax.ShapeDtypeStruct(a.shape, a.dtype)
    return pl.pallas_call(
        next_kernel,
        out_shape=[jax.ShapeDtypeStruct((N_IMG, CLASSES), F32)] + [like(a) for a in (w_in, m_in, w_out, m_out, w_head, m_head)],
        in_specs=[any_space] * 8 + [smem] * 2,
        out_specs=[vmem] + [any_space] * 6,
        scratch_shapes=[
            pltpu.VMEM((CHUNKS * 256, UR, 128), BF),
            pltpu.VMEM((N_IMG * SEQ, D), BF),
            pltpu.VMEM((SLOTS, D, FF), F32),
            pltpu.VMEM((SLOTS, D, FF), F32),
            pltpu.VMEM((SLOTS, FF, D), F32),
            pltpu.VMEM((SLOTS, FF, D), F32),
            pltpu.VMEM((D, CLASSES), F32),
            pltpu.VMEM((D, CLASSES), F32),
            pltpu.VMEM((D, FF), BF),
            pltpu.VMEM((FF, D), BF),
            pltpu.VMEM((D, CLASSES), BF),
            pltpu.VMEM((16, D), F32),
            pltpu.SemaphoreType.DMA((LAYERS + 2,)),
            pltpu.SemaphoreType.DMA((LAYERS + 1, 4)),
            pltpu.SemaphoreType.DMA((LAYERS + 1, 4)),
        ],
        compiler_params=pltpu.CompilerParams(vmem_limit_bytes=67043328),
        name='update_and_next',
    )(g, x, w_in, m_in, w_out, m_out, w_head, m_head, lr, coef)


def solution(mesh):
    def local_step(x_step, labels, x_next, w_in, w_out, w_head, mom_in, mom_out, mom_head, learn_rate, mom_coef):
        lab = jnp.pad(labels.reshape(IMGS, 1), ((0, 16 - IMGS), (0, 0)), constant_values=-1)
        g = summed_gradients(x_step.reshape(TOK, D), lab, w_in, w_out, w_head)
        logits, nwi, nmi, nwo, nmo, nwh, nmh = update_and_next(
            g, x_next.reshape(N_IMG * SEQ, D), w_in, mom_in, w_out, mom_out, w_head, mom_head,
            learn_rate.reshape(1), mom_coef.reshape(1))
        return logits, nwi, nwo, nwh, nmi, nmo, nmh

    rep3 = P(None, None, None)
    rep2 = P(None, None)
    return jax.shard_map(
        local_step, mesh=mesh,
        in_specs=(P(None, 'data', None, None), P(None, 'data'), P('data', None, None),
                  rep3, rep3, rep2, rep3, rep3, rep2, P(), P()),
        out_specs=(P('data', None), rep3, rep3, rep2, rep3, rep3, rep2),
        check_vma=False)
```
